32 devices in a mesh: rep: 4 (over x, core), fsdp: 8 (over z, y).
Axes of the slice: x: 2, y: 2, z: 4, core: 2. Of those that a mesh axis runs over, the one named last changes fastest.
Arguments:
- features: bfloat16 [4096, 1280], P(('rep', 'fsdp')), may hold values from -6 to 6
- cotangent: bfloat16 [4096, 1280], P(('rep', 'fsdp')), may hold values from -1 to 1
- clip_lengths: int32 [4, 8], P('rep'), may hold values from 96 to 128, as said below
- group_clips: int32 [4], P('rep'), may hold values from 6 to 8, as said below
- outer_attention: float32 [2, 1280, 5120], P(None, 'fsdp')
- outer_feedforward: float32 [2, 1280, 10240], P(None, 'fsdp')
- outer_vectors: float32 [2, 12, 1280], P(None, None, 'fsdp')
- moments_attention: float32 [4, 2, 1280, 5120], P('rep', None, 'fsdp')
- moments_feedforward: float32 [4, 2, 1280, 10240], P('rep', None, 'fsdp')
- moments_vectors: float32 [4, 2, 12, 1280], P('rep', None, None, 'fsdp')
Outputs:
- block_output: bfloat16 [4096, 1280], P(('rep', 'fsdp'))
- input_grad: float32 [4096, 1280], P(('rep', 'fsdp'))
- group_attention: float32 [4, 3, 1280, 5120], P('rep', None, 'fsdp')
- group_feedforward: float32 [4, 3, 1280, 10240], P('rep', None, 'fsdp')
- group_vectors: float32 [4, 3, 12, 1280], P('rep', None, None, 'fsdp')
- group_weights: float32 [4, 1280, 15372], P('rep', 'fsdp')
- next_attention: float32 [3, 1280, 5120], P(None, 'fsdp')
- next_feedforward: float32 [3, 1280, 10240], P(None, 'fsdp')
- next_vectors: float32 [3, 12, 1280], P(None, None, 'fsdp')
- copy_attention: bfloat16 [1280, 5120], P('fsdp')
- copy_feedforward: bfloat16 [1280, 10240], P('fsdp')
- copy_vectors: bfloat16 [12, 1280], P(None, 'fsdp')
The draws below stay inside these ranges and needn't reach their ends.
Inputs may be any that keep to these rules, and one draw needn't show every extreme that they name: `clip_lengths`: some clip has exactly 128 valid tokens and some exactly 96. Group g holds clips in its slots 0 to group_clips[g] - 1 and none in the others; some group has all 8 and some 8 - 2.
All inputs are finite; a program needn't handle non-finite values.
Results may differ from the reference program's by a relative error of at most 0.012.
The reference program's roundings to bfloat16 on the way count: a program that leaves them out, or rounds other values in their place, can miss the bound.
Values may be sent and summed in bfloat16 or wider, within the bound.
A program may use at most 448 MiB of HBM per device.

```python
import jax
import jax.numpy as jnp
from jax import lax

D = 1280
HEADS = 16
HD = 80
FF = 5120
STEP = 3
LEN = 128
SLOTS = 8
ROWS = 4096
N_REP = 4


def normal_or_flat(key, shape):
    return jnp.clip(jax.random.normal(key, shape, jnp.float32), -6.0, 6.0)


def moment_pair(key, shape):
    size_key, spread_key = jax.random.split(key)
    grad_scale = 0.5
    first_moment = grad_scale * normal_or_flat(size_key, (N_REP,) + shape)
    spread = jnp.exp(jax.random.uniform(spread_key, (N_REP,) + shape, jnp.float32, -1.2, 1.2))
    second_moment = (grad_scale * spread) ** 2
    return jnp.stack([first_moment, second_moment], axis=1)


def draw_cotangent(key, part):
    value_key = jax.random.fold_in(key, 41)
    return (normal_or_flat(value_key, (ROWS, D)) * (SLOTS * LEN) ** (-0.5)).astype(jnp.bfloat16)


def draw_outer_attention(key, part):
    weight_key, moment_key = jax.random.split(jax.random.fold_in(key, 11))
    columns = jnp.arange(4 * D)
    factor = jnp.where(columns < 2 * D, 1.25, jnp.where(columns < 3 * D, 1.0, 7.0)) * D ** (-0.5)
    weights = normal_or_flat(weight_key, (D, 4 * D)) * factor[None, :]
    momentum = 0.03 * normal_or_flat(moment_key, (D, 4 * D))
    return jnp.stack([weights, momentum])


def draw_outer_feedforward(key, part):
    weight_key, moment_key = jax.random.split(jax.random.fold_in(key, 12))
    columns = jnp.arange(2 * FF)
    factor = jnp.where(columns < FF, D ** (-0.5), 1.5 * FF ** (-0.5))
    weights = normal_or_flat(weight_key, (D, 2 * FF)) * factor[None, :]
    momentum = 0.03 * normal_or_flat(moment_key, (D, 2 * FF))
    return jnp.stack([weights, momentum])


def draw_outer_vectors(key, part):
    gain_key, bias_key, moment_key = jax.random.split(jax.random.fold_in(key, 13), 3)
    row_index = jnp.arange(12)[:, None]
    gain_values = jax.random.uniform(gain_key, (12, D), jnp.float32, 0.5, 1.5)
    biases = 0.5 * normal_or_flat(bias_key, (12, D))
    vectors = jnp.where((row_index == 0) | (row_index == 5), gain_values, biases)
    momentum = 0.03 * normal_or_flat(moment_key, (12, D))
    return jnp.stack([vectors, momentum])


def draw_moments_attention(key, part):
    return moment_pair(jax.random.fold_in(key, 21), (D, 4 * D))


def draw_moments_feedforward(key, part):
    return moment_pair(jax.random.fold_in(key, 22), (D, 2 * FF))


def draw_moments_vectors(key, part):
    return moment_pair(jax.random.fold_in(key, 23), (12, D))


def draw_clip_lengths(key, part):
    value_key, place_key = jax.random.split(jax.random.fold_in(key, 31))
    shortest = LEN - LEN // 4
    drawn_lengths = jax.random.randint(value_key, (N_REP * SLOTS,), shortest, LEN + 1)
    ordering = jax.random.permutation(place_key, N_REP * SLOTS)
    drawn_lengths = drawn_lengths.at[ordering[0]].set(LEN).at[ordering[1]].set(shortest)
    return drawn_lengths.reshape(N_REP, SLOTS).astype(jnp.int32)


def draw_group_clips(key, part):
    value_key, place_key = jax.random.split(jax.random.fold_in(key, 32))
    counts = SLOTS - jax.random.randint(value_key, (N_REP,), 0, 3)
    ordering = jax.random.permutation(place_key, N_REP)
    counts = counts.at[ordering[0]].set(SLOTS).at[ordering[1]].set(SLOTS - 2)
    return counts.astype(jnp.int32)


def level_of(rng, shape, pieces, smallest, largest):
    level, own = 1.0, jax.random.fold_in(rng, 6)
    for axis_at, blocks in pieces:
        heights = jnp.exp(jax.random.uniform(jax.random.fold_in(own, axis_at), (blocks,), jnp.float32, smallest / len(pieces), largest / len(pieces)))
        level = level * jnp.repeat(heights, shape[axis_at] // blocks).reshape([-1 if axis == axis_at else 1 for axis in range(len(shape))])
    return level


def noise(own_key, shape, scale, bound, pieces=(), held_as=jnp.bfloat16):
    drawn = scale * jax.random.normal(own_key, shape, jnp.float32)
    if pieces:
        drawn = drawn * level_of(own_key, shape, pieces, -0.22, 0.18)
    return jnp.clip(drawn, -bound, bound).astype(held_as)


def setup_inputs(seed: int = 0) -> dict:
    key_list = jax.random.split(jax.random.key(seed), 11)
    return {
        "features": noise(key_list[0], (ROWS, D), 1.0, 6.0, ((0, 32),)),
        "cotangent": draw_cotangent(jax.random.fold_in(key_list[10], 71), 0),
        "clip_lengths": draw_clip_lengths(jax.random.fold_in(key_list[10], 71), 0),
        "group_clips": draw_group_clips(jax.random.fold_in(key_list[10], 71), 0),
        "outer_attention": draw_outer_attention(jax.random.fold_in(key_list[10], 71), 0),
        "outer_feedforward": draw_outer_feedforward(jax.random.fold_in(key_list[10], 71), 0),
        "outer_vectors": draw_outer_vectors(jax.random.fold_in(key_list[10], 71), 0),
        "moments_attention": draw_moments_attention(jax.random.fold_in(key_list[10], 71), 0),
        "moments_feedforward": draw_moments_feedforward(jax.random.fold_in(key_list[10], 71), 0),
        "moments_vectors": draw_moments_vectors(jax.random.fold_in(key_list[10], 71), 0),
    }


@jax.custom_vjp
def low(v):
    return lax.optimization_barrier(v.astype(jnp.bfloat16)).astype(jnp.float32)

@jax.custom_vjp
def low_back(v):
    return v

def low_keep(v):
    return (low(v), None)

def low_pass(kept, grad):
    return (grad,)

def back_keep(v):
    return (v, None)

def back_low(kept, grad):
    return (low(grad),)
low.defvjp(low_keep, low_pass)
low_back.defvjp(back_keep, back_low)
HIGHEST = lax.Precision.HIGHEST
NORM_EPS = 1e-05
MASKED = -1e+30
ADAM_RATE = 0.03
ADAM_DECAY = 0.1
ADAM_BETA = 0.5
ADAM_EPS = 1e-08
OUTER_RATE = 0.7
OUTER_MOMENTUM = 0.5

def matmul(left, right):
    return jnp.dot(left, right, precision=HIGHEST, preferred_element_type=jnp.float32)

def matmul_transposed(left, right):
    return lax.dot_general(left, right, (((1,), (1,)), ((), ())), precision=HIGHEST, preferred_element_type=jnp.float32)

def layer_norm(inputs, gain_row, shift_row):
    average = lax.optimization_barrier(jnp.mean(inputs, axis=-1, keepdims=True))
    centered = inputs - average
    variance = lax.optimization_barrier(jnp.mean(centered * centered, axis=-1, keepdims=True))
    return centered * lax.rsqrt(variance + NORM_EPS) * gain_row + shift_row

def clip_forward(params, inputs, clip_length):
    w_attention, w_feedforward, vectors = params
    layer_one = low(layer_norm(inputs, vectors[0], vectors[1]))
    qkv_bias = jnp.concatenate([vectors[2], jnp.zeros_like(vectors[2]), vectors[3]])
    projected = low_back(low(matmul(layer_one, w_attention[:, :3 * D]) + qkv_bias))
    query_blocks = projected[:, :D].reshape(1, LEN, HEADS, HD)
    key_heads = projected[:, D:2 * D].reshape(LEN, HEADS, HD)
    value_heads = projected[:, 2 * D:].reshape(LEN, HEADS, HD)
    key_valid = jnp.arange(LEN) < clip_length

    def query_block(block_rows):
        scores = jnp.einsum('qhd,khd->hqk', block_rows, key_heads, precision=HIGHEST) * HD ** (-0.5)
        scores = jnp.where(key_valid[None, None, :], low_back(scores), MASKED)
        top_score = lax.optimization_barrier(jnp.max(scores, axis=-1, keepdims=True))
        exponent = jnp.exp(scores - top_score)
        attention_probs = exponent / lax.optimization_barrier(jnp.sum(exponent, axis=-1, keepdims=True))
        return jnp.einsum('hqk,khd->qhd', low(attention_probs), value_heads, precision=HIGHEST)
    attended = lax.map(jax.checkpoint(query_block), query_blocks).reshape(LEN, D)
    attended = low_back(low(attended))
    attention_branch = low_back(matmul_transposed(attended, w_attention[:, 3 * D:]) + vectors[4])
    middle = inputs + attention_branch
    layer_two = low(layer_norm(middle, vectors[5], vectors[6]))
    pre_activation = low_back(matmul(layer_two, w_feedforward[:, :FF]) + vectors[8:].reshape(FF))
    activation = low(jax.nn.gelu(pre_activation, approximate=False))
    feedforward_branch = low_back(matmul_transposed(activation, w_feedforward[:, FF:]) + vectors[7])
    return middle + feedforward_branch

def group_forward(params, clips, lengths_row):

    def one_clip(carried, item_pair):
        return (carried, jax.checkpoint(clip_forward)(params, item_pair[0], item_pair[1]))
    unused, outputs = lax.scan(one_clip, jnp.zeros((), jnp.float32), (clips, lengths_row))
    return outputs

def adamw_step(weight, gradient, moments, decay_rate):
    first_moment = ADAM_BETA * moments[0] + (1.0 - ADAM_BETA) * gradient
    second_moment = ADAM_BETA * moments[1] + (1.0 - ADAM_BETA) * gradient * gradient
    correction = 1.0 - ADAM_BETA ** STEP
    direction = first_moment / correction / (jnp.sqrt(second_moment / correction) + ADAM_EPS)
    return (weight - ADAM_RATE * (direction + decay_rate * weight), first_moment, second_moment)

def outer_step(master, mean_delta, momentum_old):
    momentum = OUTER_MOMENTUM * momentum_old - mean_delta
    outer_next = master - OUTER_RATE * (OUTER_MOMENTUM * momentum - mean_delta)
    return (jnp.stack([mean_delta, momentum, outer_next]), outer_next.astype(jnp.bfloat16))

def reference(features, cotangent, clip_lengths, group_clips, outer_attention, outer_feedforward, outer_vectors, moments_attention, moments_feedforward, moments_vectors):
    masters = (outer_attention[0], outer_feedforward[0], outer_vectors[0])
    params = tuple((master.astype(jnp.bfloat16).astype(jnp.float32) for master in masters))
    positions = jnp.arange(LEN)
    slot_index = jnp.arange(SLOTS)
    group_rows = SLOTS * LEN
    outputs = []
    input_grads = []
    gradients = []
    for group_index in range(N_REP):
        rows_from = group_index * group_rows
        clips = features[rows_from:rows_from + group_rows].astype(jnp.float32).reshape(SLOTS, LEN, D)
        upstream = cotangent[rows_from:rows_from + group_rows].astype(jnp.float32).reshape(SLOTS, LEN, D)
        lengths_row = clip_lengths[group_index]
        row_valid = (positions[None, :] < lengths_row[:, None]) & (slot_index[:, None] < group_clips[group_index])
        upstream = upstream * row_valid[:, :, None].astype(jnp.float32)
        result, backward = jax.vjp(lambda weights, inputs: group_forward(weights, inputs, lengths_row), params, clips)
        grad_params, grad_inputs = backward(upstream)
        outputs.append(result.reshape(group_rows, D))
        input_grads.append(grad_inputs.reshape(group_rows, D))
        gradients.append(grad_params)
    block_output = jnp.concatenate(outputs, axis=0).astype(jnp.bfloat16)
    input_grad = jnp.concatenate(input_grads, axis=0)
    moments_all = (moments_attention, moments_feedforward, moments_vectors)
    outers = (outer_attention, outer_feedforward, outer_vectors)
    decays = (ADAM_DECAY, ADAM_DECAY, 0.0)
    group_outs = []
    next_outs = []
    copy_outs = []
    updated_all = []
    for member in range(3):
        master = masters[member]
        stacked = []
        deltas = []
        updated_list = []
        for group_index in range(N_REP):
            grad_here = gradients[group_index][member]
            updated, first_moment, second_moment = adamw_step(master, grad_here, moments_all[member][group_index], decays[member])
            stacked.append(jnp.stack([grad_here, first_moment, second_moment]))
            deltas.append(updated - master)
            updated_list.append(updated)
        mean_delta = sum(deltas) / N_REP
        next_state, copy_state = outer_step(master, mean_delta, outers[member][1])
        group_outs.append(jnp.stack(stacked))
        next_outs.append(next_state)
        copy_outs.append(copy_state)
        updated_all.append(updated_list)
    group_weights = jnp.stack([jnp.concatenate([updated_all[0][group_index], updated_all[1][group_index], updated_all[2][group_index].T], axis=1) for group_index in range(N_REP)])
    return (block_output, input_grad, group_outs[0], group_outs[1], group_outs[2], group_weights, next_outs[0], next_outs[1], next_outs[2], copy_outs[0], copy_outs[1], copy_outs[2])
```

```python
from functools import partial

import jax
import jax.numpy as jnp
from jax import lax
from jax.experimental import pallas as pl
from jax.experimental.pallas import tpu as pltpu
from jax.sharding import PartitionSpec as P

D = 1280
HEADS = 16
HD = 80
FF = 5120
STEP = 3


NORM_EPS = 1e-05
MASKED = -1e30
ADAM_RATE = 0.03
ADAM_DECAY = 0.1
ADAM_BETA = 0.5
ADAM_EPS = 1e-08
OUTER_RATE = 0.7
OUTER_MOMENTUM = 0.5


def contract_last(left, right):
    return lax.dot_general(
        left, right, (((1,), (1,)), ((), ())), preferred_element_type=jnp.float32
    )


def contract_rows(left, right):
    return lax.dot_general(
        left, right, (((0,), (0,)), ((), ())), preferred_element_type=jnp.float32
    )


def normalize(inputs, gain_row, shift_row):
    average = jnp.mean(inputs, axis=-1, keepdims=True)
    centered = inputs - average
    reciprocal = lax.rsqrt(jnp.mean(centered * centered, axis=-1, keepdims=True) + NORM_EPS)
    unit_rows = centered * reciprocal
    return (unit_rows * gain_row + shift_row, unit_rows, reciprocal)


def normalize_back(incoming, unit_rows, reciprocal, gain_row):
    scaled = incoming * gain_row
    centered = scaled - jnp.mean(scaled, axis=-1, keepdims=True)
    return reciprocal * (
        centered - unit_rows * jnp.mean(scaled * unit_rows, axis=-1, keepdims=True)
    )


def adamw_step(weight, gradient, moments, decay_rate):
    first_moment = ADAM_BETA * moments[0] + (1.0 - ADAM_BETA) * gradient
    second_moment = ADAM_BETA * moments[1] + (1.0 - ADAM_BETA) * gradient * gradient
    correction = 1.0 - ADAM_BETA**STEP
    direction = first_moment / correction / (jnp.sqrt(second_moment / correction) + ADAM_EPS)
    return (weight - ADAM_RATE * (direction + decay_rate * weight), first_moment, second_moment)


def outer_step(master, mean_delta, momentum_old):
    momentum = OUTER_MOMENTUM * momentum_old - mean_delta
    outer_next = master - OUTER_RATE * (OUTER_MOMENTUM * momentum - mean_delta)
    return jnp.stack([mean_delta, momentum, outer_next])


def shards_generic(
    features,
    cotangent,
    clip_lengths,
    group_clips,
    outer_attention,
    outer_feedforward,
    outer_vectors,
    moments_attention,
    moments_feedforward,
    moments_vectors,
):
    tokens_here = features.shape[0]
    scale = HD ** (-0.5)
    clip_slot = lax.axis_index("fsdp")
    clip_length = lax.dynamic_index_in_dim(clip_lengths[0], clip_slot, keepdims=False)
    live_clip = clip_slot < group_clips[0]
    positions = jnp.arange(tokens_here, dtype=jnp.int32)
    key_valid = positions < clip_length
    row_valid = key_valid & live_clip
    masters = (outer_attention[0], outer_feedforward[0], outer_vectors[0])
    copies = (
        masters[0].astype(jnp.bfloat16),
        masters[1].astype(jnp.bfloat16),
        masters[2].astype(jnp.bfloat16),
    )
    full_attention, full_feedforward, full_vectors = (
        lax.all_gather(copies[0], "fsdp", axis=0, tiled=True),
        lax.all_gather(copies[1], "fsdp", axis=0, tiled=True),
        lax.all_gather(copies[2], "fsdp", axis=1, tiled=True),
    )
    vectors = full_vectors.astype(jnp.float32)
    inputs = features.astype(jnp.float32)
    normed_one, unit_one, scale_one = normalize(inputs, vectors[0], vectors[1])
    layer_one = normed_one.astype(jnp.bfloat16)
    qkv_bias = jnp.concatenate([vectors[2], jnp.zeros_like(vectors[2]), vectors[3]])
    projected = (
        jnp.dot(layer_one, full_attention[:, : 3 * D], preferred_element_type=jnp.float32)
        + qkv_bias
    ).astype(jnp.bfloat16)
    query_heads = projected[:, :D].reshape(tokens_here, HEADS, HD)
    key_heads = projected[:, D : 2 * D].reshape(tokens_here, HEADS, HD)
    value_heads = projected[:, 2 * D :].reshape(tokens_here, HEADS, HD)

    def score_block():
        raw_scores = (
            jnp.einsum("qhd,khd->hqk", query_heads, key_heads, preferred_element_type=jnp.float32)
            * scale
        )
        return jnp.where(key_valid[None, None, :], raw_scores, MASKED)

    scores = score_block()
    top_score = jnp.max(scores, axis=-1, keepdims=True)
    exponent = jnp.exp(scores - top_score)
    totals = jnp.sum(exponent, axis=-1, keepdims=True)
    attention_probs = exponent / totals
    log_totals = top_score + jnp.log(totals)
    attended = jnp.einsum(
        "hqk,khd->qhd",
        attention_probs.astype(jnp.bfloat16),
        value_heads,
        preferred_element_type=jnp.float32,
    )
    attended = attended.reshape(tokens_here, D).astype(jnp.bfloat16)
    attention_branch = contract_last(attended, full_attention[:, 3 * D :]) + vectors[4]
    middle = inputs + attention_branch
    normed_two, unit_two, scale_two = normalize(middle, vectors[5], vectors[6])
    layer_two = normed_two.astype(jnp.bfloat16)
    pre_activation = jnp.dot(
        layer_two, full_feedforward[:, :FF], preferred_element_type=jnp.float32
    ) + vectors[8:].reshape(FF)
    activation, gelu_backward = jax.vjp(partial(jax.nn.gelu, approximate=False), pre_activation)
    activation_low = activation.astype(jnp.bfloat16)
    feedforward_branch = contract_last(activation_low, full_feedforward[:, FF:]) + vectors[7]
    block_output = (middle + feedforward_branch).astype(jnp.bfloat16)
    back_attention, back_feedforward, back_vectors = (
        lax.all_gather(copies[0], "fsdp", axis=0, tiled=True),
        lax.all_gather(copies[1], "fsdp", axis=0, tiled=True),
        lax.all_gather(copies[2], "fsdp", axis=1, tiled=True),
    )
    gain_rows = back_vectors.astype(jnp.float32)
    upstream = cotangent.astype(jnp.float32) * row_valid[:, None].astype(jnp.float32)
    upstream_low = upstream.astype(jnp.bfloat16)
    grad_down_bias = jnp.sum(upstream_low, axis=0, dtype=jnp.float32)
    grad_activation = jnp.dot(
        upstream_low, back_feedforward[:, FF:], preferred_element_type=jnp.float32
    )
    grad_pre = gelu_backward(grad_activation)[0].astype(jnp.bfloat16)
    grad_up_bias = jnp.sum(grad_pre, axis=0, dtype=jnp.float32)
    grad_two = contract_last(grad_pre, back_feedforward[:, :FF])
    grad_gain_two = jnp.sum(grad_two * unit_two, axis=0)
    grad_shift_two = jnp.sum(grad_two, axis=0)
    grad_middle = upstream + normalize_back(grad_two, unit_two, scale_two, gain_rows[5])
    middle_low = grad_middle.astype(jnp.bfloat16)
    grad_out_bias = jnp.sum(middle_low, axis=0, dtype=jnp.float32)
    grad_attended = jnp.dot(
        middle_low, back_attention[:, 3 * D :], preferred_element_type=jnp.float32
    ).astype(jnp.bfloat16)
    grad_heads = grad_attended.reshape(tokens_here, HEADS, HD)
    attention_probs = jnp.exp(score_block() - log_totals)
    grad_probs = jnp.einsum(
        "qhd,khd->hqk", grad_heads, value_heads, preferred_element_type=jnp.float32
    )
    row_dot = jnp.sum(attention_probs * grad_probs, axis=-1, keepdims=True)
    grad_scores = (attention_probs * (grad_probs - row_dot)).astype(jnp.bfloat16)
    grad_queries = (
        jnp.einsum("hqk,khd->qhd", grad_scores, key_heads, preferred_element_type=jnp.float32)
        * scale
    ).reshape(tokens_here, D)
    grad_keys = (
        jnp.einsum("hqk,qhd->khd", grad_scores, query_heads, preferred_element_type=jnp.float32)
        * scale
    ).reshape(tokens_here, D)
    grad_values = jnp.einsum(
        "hqk,qhd->khd",
        attention_probs.astype(jnp.bfloat16),
        grad_heads,
        preferred_element_type=jnp.float32,
    ).reshape(tokens_here, D)
    grad_qkv = jnp.concatenate([grad_queries, grad_keys, grad_values], axis=1).astype(jnp.bfloat16)
    grad_query_bias = jnp.sum(grad_qkv[:, :D], axis=0, dtype=jnp.float32)
    grad_value_bias = jnp.sum(grad_qkv[:, 2 * D :], axis=0, dtype=jnp.float32)
    grad_one = contract_last(grad_qkv, back_attention[:, : 3 * D])
    grad_gain_one = jnp.sum(grad_one * unit_one, axis=0)
    grad_shift_one = jnp.sum(grad_one, axis=0)
    input_grad = grad_middle + normalize_back(grad_one, unit_one, scale_one, gain_rows[0])
    vector_rows = jnp.stack(
        [
            grad_gain_one,
            grad_shift_one,
            grad_query_bias,
            grad_value_bias,
            grad_out_bias,
            grad_gain_two,
            grad_shift_two,
            grad_down_bias,
        ]
    )
    grad_vectors = jnp.concatenate([vector_rows, grad_up_bias.reshape(4, D)], axis=0)
    owned_attention = lax.psum_scatter(
        jnp.concatenate(
            [contract_rows(layer_one, grad_qkv), contract_rows(middle_low, attended)], axis=1
        ),
        "fsdp",
        scatter_dimension=0,
        tiled=True,
    )
    owned_feedforward = lax.psum_scatter(
        jnp.concatenate(
            [contract_rows(layer_two, grad_pre), contract_rows(upstream_low, activation_low)],
            axis=1,
        ),
        "fsdp",
        scatter_dimension=0,
        tiled=True,
    )
    owned_vectors = lax.psum_scatter(grad_vectors, "fsdp", scatter_dimension=1, tiled=True)
    new_attention, first_attention, second_attention = adamw_step(
        masters[0], owned_attention, moments_attention[0], ADAM_DECAY
    )
    new_feedforward, first_feedforward, second_feedforward = adamw_step(
        masters[1], owned_feedforward, moments_feedforward[0], ADAM_DECAY
    )
    new_vectors, first_vectors, second_vectors = adamw_step(
        masters[2], owned_vectors, moments_vectors[0], 0.0
    )
    summed = (
        lax.psum_scatter(
            (new_attention - masters[0]).astype(jnp.bfloat16),
            "rep",
            scatter_dimension=1,
            tiled=True,
        ).astype(jnp.float32),
        lax.psum_scatter(
            (new_feedforward - masters[1]).astype(jnp.bfloat16),
            "rep",
            scatter_dimension=1,
            tiled=True,
        ).astype(jnp.float32),
        lax.psum_scatter(
            (new_vectors - masters[2]).astype(jnp.bfloat16), "rep", scatter_dimension=0, tiled=True
        ).astype(jnp.float32),
    )
    replicas = lax.axis_size("rep")
    replica_index = lax.axis_index("rep")
    attention_cols = 4 * D // replicas
    feedforward_cols = 2 * FF // replicas
    vector_count = 12 // replicas

    def owned_part(array, dim, count):
        return lax.dynamic_slice_in_dim(array, replica_index * count, count, dim)

    part_attention = outer_step(
        owned_part(masters[0], 1, attention_cols),
        summed[0] / replicas,
        owned_part(outer_attention[1], 1, attention_cols),
    )
    part_feedforward = outer_step(
        owned_part(masters[1], 1, feedforward_cols),
        summed[1] / replicas,
        owned_part(outer_feedforward[1], 1, feedforward_cols),
    )
    part_vectors = outer_step(
        owned_part(masters[2], 0, vector_count),
        summed[2] / replicas,
        owned_part(outer_vectors[1], 0, vector_count),
    )
    next_attention, next_feedforward, next_vectors = (
        lax.all_gather(part_attention, "rep", axis=2, tiled=True),
        lax.all_gather(part_feedforward, "rep", axis=2, tiled=True),
        lax.all_gather(part_vectors, "rep", axis=1, tiled=True),
    )
    copy_attention = next_attention[2].astype(jnp.bfloat16)
    copy_feedforward = next_feedforward[2].astype(jnp.bfloat16)
    copy_vectors = next_vectors[2].astype(jnp.bfloat16)
    group_attention = jnp.stack([owned_attention, first_attention, second_attention])[None]
    group_feedforward = jnp.stack([owned_feedforward, first_feedforward, second_feedforward])[None]
    group_vectors = jnp.stack([owned_vectors, first_vectors, second_vectors])[None]
    group_weights = jnp.concatenate([new_attention, new_feedforward, new_vectors.T], axis=1)[None]
    return (
        block_output,
        input_grad,
        group_attention,
        group_feedforward,
        group_vectors,
        group_weights,
        next_attention,
        next_feedforward,
        next_vectors,
        copy_attention,
        copy_feedforward,
        copy_vectors,
    )


LEN = 128
TP = 8
HW = D // TP
FW = FF // TP
CW = 4 * HW + 2 * FW
AUX = 16
MESH = pl.DeviceIdType.MESH
BF = jnp.bfloat16
F32 = jnp.float32


def place():
    r, f = lax.axis_index("rep"), lax.axis_index("fsdp")
    x, k, c, q = r // 2, r % 2, f // 4, f % 4
    return r, f, x, k, c, q, 4 * k + q


def flip(q, j):
    low, high = q % 2, q // 2
    if j & 1:
        low = 1 - low
    if j & 2:
        high = 1 - high
    return high * 2 + low


def remote(src, dst, send, recv, rep, fsdp):
    return pltpu.make_async_remote_copy(
        src_ref=src,
        dst_ref=dst,
        send_sem=send,
        recv_sem=recv,
        device_id={"rep": rep, "fsdp": fsdp},
        device_id_type=MESH,
    )


def meet(peers):
    barrier = pltpu.get_barrier_semaphore()
    for rep, fsdp in peers:
        pl.semaphore_signal(
            barrier, inc=1, device_id={"rep": rep, "fsdp": fsdp}, device_id_type=MESH
        )
    pl.semaphore_wait(barrier, len(peers))


def comm_params(cid):
    return pltpu.CompilerParams(collective_id=cid, has_side_effects=True)


ANY = pl.BlockSpec(memory_space=pl.ANY)
VM = pl.BlockSpec(memory_space=pltpu.VMEM)
DMA = pltpu.SemaphoreType.DMA


def first_kernel(x_ref, u_ref, w_ref, v_ref, xf, uf, wf, vf, own, sw, rw, ls, sg, rg, sp, rp, sv, rv, so, ro, fo, go):
    r, f, x, k, c, q, w = place()
    peers = [(2 * x + (k + kk) % 2, (f + i) % 8) for kk in range(2) for i in range(8) if kk or i]
    meet(peers + [(2 * (1 - x) + k, f)])
    pr, pf = 2 * x + c, 4 * k + q
    swaps = [
        remote(src, dst.at[f], sw.at[n], rw.at[n], pr, pf)
        for n, (src, dst) in enumerate(((x_ref, xf), (u_ref, uf)))
    ]
    keeps = [
        pltpu.make_async_copy(src, dst.at[w], ls.at[n])
        for n, (src, dst) in enumerate(((x_ref, xf), (u_ref, uf)))
    ]

    @pl.when(k != c)
    def _():
        for copy in swaps:
            copy.start()

    @pl.when(k == c)
    def _():
        for copy in keeps:
            copy.start()

    half = pl.ds(pl.multiple_of(x * (HW // 2), 16), HW // 2)
    sends = []
    for i in range(1, 8):
        to = (f + i) % 8
        vec = remote(v_ref, vf.at[f], sv.at[i], rv.at[i], r, to)
        vec.start()
        out = remote(w_ref.at[to % 4, half], wf.at[f, half], so.at[i], ro.at[i], r, to)
        out.start()
        sends += [vec, out]
    load = pltpu.make_async_copy(w_ref.at[q], own, ls.at[2])
    load.start()
    keep_vec = pltpu.make_async_copy(v_ref, vf.at[f], ls.at[3])
    keep_vec.start()
    load.wait()
    keep_own = pltpu.make_async_copy(own, wf.at[f], ls.at[4])
    keep_own.start()

    partner = 2 * x + 1 - k
    spread = []
    for n, dst in enumerate((xf, uf)):

        @pl.when(k != c)
        def _(n=n):
            swaps[n].wait_recv()

        @pl.when(k == c)
        def _(n=n):
            keeps[n].wait()

        mine = dst.at[w]
        to_partner = remote(mine, mine, sp.at[n, 0], rp.at[n, 0], partner, f)
        to_partner.start()
        near = [
            remote(mine, mine, sg.at[n, j], rg.at[n, j], r, 4 * c + flip(q, j)) for j in range(1, 4)
        ]
        for copy in near:
            copy.start()
        spread.append((dst, near, [to_partner]))
    for n, (dst, near, passed) in enumerate(spread):
        for j in range(1, 4):
            near[j - 1].wait_recv()
            got = dst.at[4 * k + flip(q, j)]
            copy = remote(got, got, sp.at[n, j], rp.at[n, j], partner, f)
            copy.start()
            passed.append(copy)
    over = []
    for i in range(1, 8):
        source = (f + 8 - i) % 8
        sends[2 * i - 1].wait_recv()
        got = wf.at[source, half]
        copy = remote(got, got, fo.at[i], go.at[i], 2 * (1 - x) + k, f)
        copy.start()
        over.append(copy)
    for dst, near, passed in spread:
        for copy in near:
            copy.wait_send()
        for copy in passed:
            copy.wait()
    for i in range(1, 8):
        sends[2 * i - 2].wait()
        sends[2 * i - 1].wait_send()
    for copy in over:
        copy.wait()
    keep_vec.wait()
    keep_own.wait()

    @pl.when(k != c)
    def _():
        for copy in swaps:
            copy.wait_send()


def first_exchange(xb, ub, wsend, vsend):
    return pl.pallas_call(
        first_kernel,
        name="first_exchange",
        out_shape=(
            jax.ShapeDtypeStruct((TP,) + xb.shape, BF),
            jax.ShapeDtypeStruct((TP,) + ub.shape, BF),
            jax.ShapeDtypeStruct((TP, HW, CW), BF),
            jax.ShapeDtypeStruct((TP,) + vsend.shape, BF),
        ),
        in_specs=[VM, VM, ANY, VM],
        out_specs=(ANY,) * 4,
        scratch_shapes=[
            pltpu.VMEM((HW, CW), BF),
            DMA((2,)),
            DMA((2,)),
            DMA((5,)),
            DMA((2, 4)),
            DMA((2, 4)),
            DMA((2, 4)),
            DMA((2, 4)),
            DMA((8,)),
            DMA((8,)),
            DMA((8,)),
            DMA((8,)),
            DMA((8,)),
            DMA((8,)),
        ],
        compiler_params=comm_params(1),
    )(xb, ub, wsend, vsend)


def gather_kernel(y_ref, out, ls, sg, rg, sp, rp):
    r, f, x, k, c, q, w = place()
    partner = 2 * x + 1 - k
    near_ids = [4 * c + flip(q, j) for j in range(1, 4)]
    meet([(r, n) for n in near_ids] + [(partner, f)])
    keep = pltpu.make_async_copy(y_ref, out.at[w], ls.at[0])
    keep.start()
    near = [
        remote(y_ref, out.at[w], sg.at[j], rg.at[j], r, near_ids[j - 1]) for j in range(1, 4)
    ]
    for copy in near:
        copy.start()
    passed = [remote(y_ref, out.at[w], sp.at[0], rp.at[0], partner, f)]
    passed[0].start()
    for j in range(1, 4):
        near[j - 1].wait_recv()
        got = out.at[4 * k + flip(q, j)]
        copy = remote(got, got, sp.at[j], rp.at[j], partner, f)
        copy.start()
        passed.append(copy)
    for copy in near:
        copy.wait_send()
    for copy in passed:
        copy.wait()
    keep.wait()


def gather_rows(y, cid):
    return pl.pallas_call(
        gather_kernel,
        name="gather_rows",
        out_shape=jax.ShapeDtypeStruct((TP,) + y.shape, y.dtype),
        in_specs=[VM],
        out_specs=ANY,
        scratch_shapes=[DMA((1,))] + [DMA((4,))] * 4,
        compiler_params=comm_params(cid),
    )(y)


def reduce_kernel(a_ref, w_ref, out, pair, got, small, far, sp, rp, sg, rg):
    r, f, x, k, c, q, w = place()
    partner = 2 * x + 1 - k
    near_ids = [4 * c + flip(q, j) for j in range(4)]
    meet([(r, n) for n in near_ids[1:]] + [(partner, f)])
    order = (3, 2, 1, 0)
    halves = []
    for j in order:
        pair[j] = contract_last(a_ref[4 * (1 - k) + flip(q, j)], w_ref[...])
        copy = remote(pair.at[j], got.at[j], sp.at[j], rp.at[j], partner, f)
        copy.start()
        halves.append(copy)
    sent = []
    total = None
    for n, j in enumerate(order):
        part = contract_last(a_ref[4 * k + flip(q, j)], w_ref[...])
        halves[n].wait_recv()
        part = part + got[j]
        if j:
            small[j] = part.astype(BF)
            copy = remote(small.at[j], far.at[j], sg.at[j], rg.at[j], r, near_ids[j])
            copy.start()
            sent.append(copy)
        else:
            total = part
    for copy in sent:
        copy.wait_recv()
    for j in order[:-1]:
        total = total + far[j].astype(F32)
    out[...] = total
    for copy in sent + halves:
        copy.wait_send()


def reduce_rows(a, weights, cid):
    return pl.pallas_call(
        reduce_kernel,
        name="reduce_rows",
        out_shape=jax.ShapeDtypeStruct((LEN, D), F32),
        in_specs=[VM, VM],
        out_specs=VM,
        scratch_shapes=[
            pltpu.VMEM((4, LEN, D), F32),
            pltpu.VMEM((4, LEN, D), F32),
            pltpu.VMEM((4, LEN, D), BF),
            pltpu.VMEM((4, LEN, D), BF),
        ]
        + [DMA((4,))] * 4,
        compiler_params=comm_params(cid),
    )(a, weights)


def first_head(shape):
    return lax.broadcasted_iota(jnp.int32, shape, 1) < HD


def attend_kernel(x_ref, m_ref, g_ref, s_ref, b_ref, w_ref, y_ref, qkv_ref, att_ref, p_ref):
    normed, _, _ = normalize(x_ref[0].astype(F32), g_ref[...], s_ref[...])
    y = normed.astype(BF)
    y_ref[0] = y
    qkv = (jnp.dot(y, w_ref[...], preferred_element_type=F32) + b_ref[...]).astype(BF)
    qkv_ref[0] = qkv
    queries, keys, values = qkv[:, :HW], qkv[:, HW : 2 * HW], qkv[:, 2 * HW :]
    valid = m_ref[0, 0:1, :LEN].astype(F32) > 0.5
    left = first_head(queries.shape)
    sums = []
    for h in range(2):
        mine = left if h == 0 else jnp.logical_not(left)
        part = jnp.where(mine, queries, jnp.zeros_like(queries))
        scores = jnp.where(valid, contract_last(part, keys) * HD ** (-0.5), MASKED)
        exponent = jnp.exp(scores - jnp.max(scores, axis=-1, keepdims=True))
        probs = exponent / jnp.sum(exponent, axis=-1, keepdims=True)
        p_ref[0, h] = probs
        sums.append(jnp.dot(probs.astype(BF), values, preferred_element_type=F32))
    att_ref[0] = jnp.where(left, sums[0], sums[1]).astype(BF)


def attend(xf, uf, gain, shift, bias, weights):
    row = lambda s: (s, 0, 0)
    whole = lambda s: (0, 0)
    return pl.pallas_call(
        attend_kernel,
        name="attend",
        grid=(TP,),
        out_shape=(
            jax.ShapeDtypeStruct((TP, LEN, D), BF),
            jax.ShapeDtypeStruct((TP, LEN, 3 * HW), BF),
            jax.ShapeDtypeStruct((TP, LEN, HW), BF),
            jax.ShapeDtypeStruct((TP, 2, LEN, LEN), F32),
        ),
        in_specs=[
            pl.BlockSpec((1, LEN, D), row),
            pl.BlockSpec((1, AUX, D), lambda s: (s, LEN // AUX, 0)),
            pl.BlockSpec((1, D), whole),
            pl.BlockSpec((1, D), whole),
            pl.BlockSpec((1, 3 * HW), whole),
            pl.BlockSpec((D, 3 * HW), whole),
        ],
        out_specs=(
            pl.BlockSpec((1, LEN, D), row),
            pl.BlockSpec((1, LEN, 3 * HW), row),
            pl.BlockSpec((1, LEN, HW), row),
            pl.BlockSpec((1, 2, LEN, LEN), lambda s: (s, 0, 0, 0)),
        ),
    )(xf, uf, gain, shift, bias, weights)


def attend_back_kernel(m_ref, wo_ref, qkv_ref, p_ref, out):
    grad = jnp.dot(m_ref[0], wo_ref[...], preferred_element_type=F32).astype(BF)
    qkv = qkv_ref[0]
    queries, keys, values = qkv[:, :HW], qkv[:, HW : 2 * HW], qkv[:, 2 * HW :]
    left = first_head(queries.shape)
    gq, gk, gv = [], [], []
    for h in range(2):
        mine = left if h == 0 else jnp.logical_not(left)
        part = jnp.where(mine, grad, jnp.zeros_like(grad))
        probs = p_ref[0, h]
        grad_probs = contract_last(part, values)
        row_dot = jnp.sum(probs * grad_probs, axis=-1, keepdims=True)
        grad_scores = (probs * (grad_probs - row_dot)).astype(BF)
        gq.append(jnp.dot(grad_scores, keys, preferred_element_type=F32))
        gk.append(contract_rows(grad_scores, queries))
        gv.append(contract_rows(probs.astype(BF), grad))
    scale = HD ** (-0.5)
    out[0, :, :HW] = (jnp.where(left, gq[0], gq[1]) * scale).astype(BF)
    out[0, :, HW : 2 * HW] = (jnp.where(left, gk[0], gk[1]) * scale).astype(BF)
    out[0, :, 2 * HW :] = jnp.where(left, gv[0], gv[1]).astype(BF)


def attend_back(middle, weights, qkv, probs):
    row = lambda s: (s, 0, 0)
    return pl.pallas_call(
        attend_back_kernel,
        name="attend_back",
        grid=(TP,),
        out_shape=jax.ShapeDtypeStruct((TP, LEN, 3 * HW), BF),
        in_specs=[
            pl.BlockSpec((1, LEN, D), row),
            pl.BlockSpec((D, HW), lambda s: (0, 0)),
            pl.BlockSpec((1, LEN, 3 * HW), row),
            pl.BlockSpec((1, 2, LEN, LEN), lambda s: (s, 0, 0, 0)),
        ],
        out_specs=pl.BlockSpec((1, LEN, 3 * HW), row),
    )(middle, weights, qkv, probs)


def units_kernel(y_ref, u_ref, up_ref, down_ref, b_ref, act_ref, grad_ref):
    pre = jnp.dot(y_ref[0], up_ref[...], preferred_element_type=F32) + b_ref[...]
    grad_act = jnp.dot(u_ref[0], down_ref[...], preferred_element_type=F32)
    below = 0.5 * (1.0 + lax.erf(pre * (0.5**0.5)))
    density = jnp.exp(-0.5 * pre * pre) * 0.3989422804014327
    act_ref[0] = (pre * below).astype(BF)
    grad_ref[0] = (grad_act * (below + pre * density)).astype(BF)


def units(y, uf, up, down, bias):
    row = lambda s: (s, 0, 0)
    whole = lambda s: (0, 0)
    return pl.pallas_call(
        units_kernel,
        name="units",
        grid=(TP,),
        out_shape=(jax.ShapeDtypeStruct((TP, LEN, FW), BF),) * 2,
        in_specs=[
            pl.BlockSpec((1, LEN, D), row),
            pl.BlockSpec((1, LEN, D), row),
            pl.BlockSpec((D, FW), whole),
            pl.BlockSpec((D, FW), whole),
            pl.BlockSpec((1, FW), whole),
        ],
        out_specs=(pl.BlockSpec((1, LEN, FW), row),) * 2,
    )(y, uf, up, down, bias)


def weight_grads_kernel(y1, mid, y2, up, gq, att, gp, act, out):
    flat = lambda ref: ref[...].reshape(TP * LEN, ref.shape[-1])
    out[:, : 3 * HW] = contract_rows(flat(y1), flat(gq)).astype(BF)
    out[:, 3 * HW : 4 * HW] = contract_rows(flat(mid), flat(att)).astype(BF)
    out[:, 4 * HW : 4 * HW + FW] = contract_rows(flat(y2), flat(gp)).astype(BF)
    out[:, 4 * HW + FW :] = contract_rows(flat(up), flat(act)).astype(BF)


def weight_grads(y1, mid, y2, uf, gq, att, gp, act):
    step = 256
    left = pl.BlockSpec((TP, LEN, step), lambda i: (0, 0, i))
    right = lambda n: pl.BlockSpec((TP, LEN, n), lambda i: (0, 0, 0))
    return pl.pallas_call(
        weight_grads_kernel,
        name="weight_grads",
        grid=(D // step,),
        out_shape=jax.ShapeDtypeStruct((D, CW), BF),
        in_specs=[left] * 4 + [right(3 * HW), right(HW), right(FW), right(FW)],
        out_specs=pl.BlockSpec((step, CW), lambda i: (i, 0)),
    )(y1, mid, y2, uf, gq, att, gp, act)


def return_kernel(g_ref, v_ref, b_ref, i_ref, gr, vr, bo, io, own, ls, sw, rw, sg, rg, sv, rv):
    r, f, x, k, c, q, w = place()
    meet([(2 * x + (k + kk) % 2, (f + i) % 8) for kk in range(2) for i in range(8) if kk or i])
    home = 2 * x + c
    pf = 4 * k + q
    swaps = [remote(b_ref, bo, sw.at[0], rw.at[0], home, pf), remote(i_ref, io, sw.at[1], rw.at[1], home, pf)]
    keeps = [pltpu.make_async_copy(b_ref, bo, ls.at[0]), pltpu.make_async_copy(i_ref, io, ls.at[1])]
    load = pltpu.make_async_copy(g_ref.at[f], own, ls.at[2])
    keep_own = pltpu.make_async_copy(own, gr.at[w], ls.at[3])
    keep_vec = pltpu.make_async_copy(v_ref.at[f], vr.at[w], ls.at[4])

    def blocks(i):
        to = (f + i) % 8
        return (
            remote(v_ref.at[to], vr.at[w], sv.at[i], rv.at[w], home, to),
            remote(g_ref.at[to], gr.at[w], sg.at[i], rg.at[w], home, to),
        )

    for i in range(1, 8):
        for copy in blocks(i):
            copy.start()

    @pl.when(k != c)
    def _():
        for copy in blocks(0):
            copy.start()
        for copy in swaps:
            copy.start()

    @pl.when(k == c)
    def _():
        for copy in keeps + [load, keep_vec]:
            copy.start()
        load.wait()
        keep_own.start()

    for kk in range(2):
        for p in range(4):
            source = 4 * kk + p

            def landed():
                remote(v_ref.at[0], vr.at[source], sv.at[0], rv.at[source], r, f).wait_recv()
                remote(g_ref.at[0], gr.at[source], sg.at[0], rg.at[source], r, f).wait_recv()

            @pl.when(jnp.logical_or(c != k, source != w))
            def _(landed=landed):
                landed()

    for i in range(1, 8):
        for copy in blocks(i):
            copy.wait_send()

    @pl.when(k != c)
    def _():
        for copy in blocks(0):
            copy.wait_send()
        for copy in swaps:
            copy.wait()

    @pl.when(k == c)
    def _():
        for copy in keeps + [keep_vec, keep_own]:
            copy.wait()


def return_exchange(grads, vecs, block, grad_in):
    shape = lambda a: jax.ShapeDtypeStruct(a.shape, a.dtype)
    return pl.pallas_call(
        return_kernel,
        name="return_exchange",
        out_shape=tuple(shape(a) for a in (grads, vecs, block, grad_in)),
        in_specs=[ANY, VM, VM, VM],
        out_specs=(ANY, VM, ANY, ANY),
        scratch_shapes=[pltpu.VMEM(grads.shape[1:], BF), DMA((5,)), DMA((2,)), DMA((2,))] + [DMA((8,))] * 4,
        compiler_params=comm_params(8),
    )(grads, vecs, block, grad_in)


def pieces():
    return [(n * HW, HW) for n in range(4)], [(4 * HW + n * FW, FW) for n in range(2)]


def adam_kernel(g_ref, wa, wf, ma, mf, nv, ga, gf, gw, da, df):
    narrow, wide = pieces()
    for parts, master, moments, grads, delta, at in (
        (narrow, wa, ma, ga, da, 0),
        (wide, wf, mf, gf, df, 4 * D),
    ):
        for n, (start, width) in enumerate(parts):
            for s in range(TP):
                grads[0, :, n * TP * width + s * width : n * TP * width + (s + 1) * width] = g_ref[
                    s, :, start : start + width
                ].astype(F32)
        weight = master[0]
        new, first, second = adamw_step(weight, grads[0], (moments[0, 0], moments[0, 1]), ADAM_DECAY)
        grads[1] = first
        grads[2] = second
        gw[:, at : at + weight.shape[1]] = new
        delta[...] = (new - weight).astype(BF)
    gw[:, 4 * D + 2 * FF :] = nv[...]


def adam(grads, outer_attention, outer_feedforward, moments_attention, moments_feedforward, new_vectors):
    step = 16
    na, nf = 4 * D, 2 * FF
    rows3 = lambda i: (0, i, 0)
    rows2 = lambda i: (i, 0)
    return pl.pallas_call(
        adam_kernel,
        name="adam",
        grid=(HW // step,),
        out_shape=(
            jax.ShapeDtypeStruct((3, HW, na), F32),
            jax.ShapeDtypeStruct((3, HW, nf), F32),
            jax.ShapeDtypeStruct((HW, na + nf + 12), F32),
            jax.ShapeDtypeStruct((HW, na), BF),
            jax.ShapeDtypeStruct((HW, nf), BF),
        ),
        in_specs=[
            pl.BlockSpec((TP, step, CW), rows3),
            pl.BlockSpec((1, step, na), rows3),
            pl.BlockSpec((1, step, nf), rows3),
            pl.BlockSpec((1, 2, step, na), lambda i: (0, 0, i, 0)),
            pl.BlockSpec((1, 2, step, nf), lambda i: (0, 0, i, 0)),
            pl.BlockSpec((step, 12), rows2),
        ],
        out_specs=(
            pl.BlockSpec((3, step, na), rows3),
            pl.BlockSpec((3, step, nf), rows3),
            pl.BlockSpec((step, na + nf + 12), rows2),
            pl.BlockSpec((step, na), rows2),
            pl.BlockSpec((step, nf), rows2),
        ),
    )(grads, outer_attention, outer_feedforward, moments_attention, moments_feedforward, new_vectors)


def groups_kernel(a_ref, f_ref, v_ref, pa, pf, qa, qf, vo, ba, bf_, vb, ss, rs, sx, rx, sf, rf, sv, rv):
    r, f, x, k, c, q, w = place()
    partner, across = 2 * x + 1 - k, 2 * (1 - x) + k
    meet([(partner, f), (across, f)])
    rows = 16
    count = HW // 2 // rows
    mine = lambda half, j: pl.ds(pl.multiple_of(half * (HW // 2) + j * rows, rows), rows)
    trio = ((a_ref, ba, pa, qa), (f_ref, bf_, pf, qf))
    vec = remote(v_ref, vb.at[0], sv.at[0], rv.at[0], partner, f)
    vec.start()
    first = {}
    for turn in range(2):
        half = (1 - k) if turn == 0 else k
        for j in range(count):
            for n, (src, buf, _, _) in enumerate(trio):
                copy = remote(src.at[mine(half, j)], buf.at[mine(half, j)], ss.at[turn, n, j], rs.at[turn, n, j], partner, f)
                copy.start()
                first[turn, n, j] = copy
    vec.wait_recv()
    vb[1] = v_ref[...] + vb[0]
    vec2 = remote(vb.at[1], vb.at[2], sv.at[1], rv.at[1], across, f)
    vec2.start()
    second = {}
    for turn in range(2):
        half = k if turn == 0 else 1 - k
        for j in range(count):
            for n, (src, buf, pair, other) in enumerate(trio):
                first[turn, n, j].wait_recv()
                at = mine(half, j)
                pair[at, :] = (src[at, :].astype(F32) + buf[at, :].astype(F32)).astype(BF)
                if turn == 0:
                    copy = remote(pair.at[at], other.at[at], sx.at[n, j], rx.at[n, j], across, f)
                    copy.start()
                    second[n, j] = copy
    third = []
    for j in range(count):
        for n, (_, _, _, other) in enumerate(trio):
            second[n, j].wait_recv()
            at = mine(k, j)
            copy = remote(other.at[at], other.at[at], sf.at[n, j], rf.at[n, j], partner, f)
            copy.start()
            third.append(copy)
    vec2.wait_recv()
    vo[...] = vb[1] + vb[2]
    for copy in third:
        copy.wait()
    for copy in list(first.values()) + list(second.values()) + [vec, vec2]:
        copy.wait_send()


def groups_sum(delta_a, delta_f, delta_v):
    count = HW // 2 // 16
    sa, sf, sv = (jax.ShapeDtypeStruct(a.shape, a.dtype) for a in (delta_a, delta_f, delta_v))
    return pl.pallas_call(
        groups_kernel,
        name="groups_sum",
        out_shape=(sa, sf, sa, sf, sv),
        in_specs=[VM] * 3,
        out_specs=(VM,) * 5,
        scratch_shapes=[
            pltpu.VMEM(delta_a.shape, BF),
            pltpu.VMEM(delta_f.shape, BF),
            pltpu.VMEM((3,) + delta_v.shape, F32),
            DMA((2, 2, count)),
            DMA((2, 2, count)),
            DMA((2, count)),
            DMA((2, count)),
            DMA((2, count)),
            DMA((2, count)),
            DMA((2,)),
            DMA((2,)),
        ],
        compiler_params=comm_params(9),
    )(delta_a, delta_f, delta_v)


def outer_kernel(pa, pf, qa, qf, oa, of, na, nf, ca, cf):
    for pair, other, outer, out, copy in ((pa, qa, oa, na, ca), (pf, qf, of, nf, cf)):
        mean = (pair[...].astype(F32) + other[...].astype(F32)) / 4
        momentum = OUTER_MOMENTUM * outer[1] - mean
        following = outer[0] - OUTER_RATE * (OUTER_MOMENTUM * momentum - mean)
        out[0] = mean
        out[1] = momentum
        out[2] = following
        copy[...] = following.astype(BF)


def outer_update(pa, pf, qa, qf, outer_attention, outer_feedforward):
    step = 16
    na, nf = 4 * D, 2 * FF
    rows2 = lambda i: (i, 0)
    rows3 = lambda i: (0, i, 0)
    two = [pl.BlockSpec((step, n), rows2) for n in (na, nf)]
    return pl.pallas_call(
        outer_kernel,
        name="outer_update",
        grid=(HW // step,),
        out_shape=(
            jax.ShapeDtypeStruct((3, HW, na), F32),
            jax.ShapeDtypeStruct((3, HW, nf), F32),
            jax.ShapeDtypeStruct((HW, na), BF),
            jax.ShapeDtypeStruct((HW, nf), BF),
        ),
        in_specs=two + two + [pl.BlockSpec((2, step, n), rows3) for n in (na, nf)],
        out_specs=tuple([pl.BlockSpec((3, step, n), rows3) for n in (na, nf)] + two),
    )(pa, pf, qa, qf, outer_attention, outer_feedforward)


def shards_split(
    features,
    cotangent,
    clip_lengths,
    group_clips,
    outer_attention,
    outer_feedforward,
    outer_vectors,
    moments_attention,
    moments_feedforward,
    moments_vectors,
):
    r, f, x, k, c, q, w = place()
    clip_length = lax.dynamic_index_in_dim(clip_lengths[0], f, keepdims=False)
    positions = jnp.arange(LEN, dtype=jnp.int32)
    key_valid = positions < clip_length
    row_valid = key_valid & (f < group_clips[0])
    up_here = jnp.where(row_valid[:, None], cotangent, jnp.zeros_like(cotangent))
    flags = jnp.broadcast_to(jnp.pad(key_valid.astype(BF), (0, D - LEN))[None], (AUX, D))
    ub = jnp.concatenate([up_here, flags], axis=0)
    part_a = outer_attention[0].astype(BF).reshape(HW, 4, 2, 4, HW)
    part_f = outer_feedforward[0].astype(BF).reshape(HW, 2, 2, 4, FW)
    part_a = lax.dynamic_index_in_dim(part_a, k, 2, keepdims=False).transpose(2, 0, 1, 3)
    part_f = lax.dynamic_index_in_dim(part_f, k, 2, keepdims=False).transpose(2, 0, 1, 3)
    wsend = jnp.concatenate([part_a.reshape(4, HW, 4 * HW), part_f.reshape(4, HW, 2 * FW)], axis=2)
    vsend = jnp.pad(outer_vectors[0].astype(BF), ((0, 4), (0, 96)))
    xf, uf, wf, vf = first_exchange(features, ub, wsend, vsend)
    vectors = vf[:, :12, :HW].transpose(1, 0, 2).reshape(12, D).astype(F32)
    columns = wf.reshape(D, CW)
    w_qkv, w_out = columns[:, : 3 * HW], columns[:, 3 * HW : 4 * HW]
    w_up, w_down = columns[:, 4 * HW : 4 * HW + FW], columns[:, 4 * HW + FW :]
    own = lambda row, width: lax.dynamic_slice_in_dim(row, w * width, width, 0)
    bias_qkv = jnp.concatenate([own(vectors[2], HW), jnp.zeros((HW,), F32), own(vectors[3], HW)])[None]
    bias_up = own(vectors[8:].reshape(FF), FW)[None]
    x_own = lax.dynamic_index_in_dim(xf, w, keepdims=False).astype(F32)
    up_own = lax.dynamic_index_in_dim(uf, w, keepdims=False)[:LEN]
    upstream = up_own.astype(F32)
    _, unit_one, scale_one = normalize(x_own, vectors[0], vectors[1])

    y1, qkv, attended, probs = attend(xf, uf, vectors[0:1], vectors[1:2], bias_qkv, w_qkv)
    middle = x_own + (reduce_rows(attended, w_out, 2) + vectors[4])
    normed_two, unit_two, scale_two = normalize(middle, vectors[5], vectors[6])
    y2 = gather_rows(normed_two.astype(BF), 3)
    act, grad_pre = units(y2, uf, w_up, w_down, bias_up)
    block_output = (middle + (reduce_rows(act, w_down, 4) + vectors[7])).astype(BF)
    grad_two = reduce_rows(grad_pre, w_up, 5)
    grad_middle = upstream + normalize_back(grad_two, unit_two, scale_two, vectors[5])
    middle_low = grad_middle.astype(BF)
    mid = gather_rows(middle_low, 6)
    grad_qkv = attend_back(mid, w_out, qkv, probs)
    grad_one = reduce_rows(grad_qkv, w_qkv, 7)
    input_grad = grad_middle + normalize_back(grad_one, unit_one, scale_one, vectors[0])
    grads = weight_grads(y1, mid, y2, uf, grad_qkv, attended, grad_pre, act).reshape(TP, HW, CW)

    total = lambda a: jnp.sum(a, axis=0, dtype=F32)
    sums_qkv = total(grad_qkv.reshape(TP * LEN, 3 * HW))
    spread = lambda part, size: lax.dynamic_update_slice_in_dim(
        jnp.zeros((size,), F32), part, w * part.shape[0], 0
    )
    rows = jnp.stack(
        [
            total(grad_one * unit_one),
            total(grad_one),
            spread(sums_qkv[:HW], D),
            spread(sums_qkv[2 * HW :], D),
            total(middle_low),
            total(grad_two * unit_two),
            total(grad_two),
            total(up_own),
        ]
    )
    partial_vectors = jnp.concatenate(
        [rows, spread(total(grad_pre.reshape(TP * LEN, FW)), FF).reshape(4, D)], axis=0
    )
    vec_send = jnp.pad(partial_vectors.reshape(12, TP, HW).transpose(1, 0, 2), ((0, 0), (0, 4), (0, 96)))
    grads_in, vecs_in, block_home, grad_home = return_exchange(grads, vec_send, block_output, input_grad)
    owned_vectors = jnp.sum(vecs_in, axis=0)[:12, :HW]
    new_vectors, first_vectors, second_vectors = adamw_step(
        outer_vectors[0], owned_vectors, moments_vectors[0], 0.0
    )
    group_a, group_f, group_w, delta_a, delta_f = adam(
        grads_in, outer_attention, outer_feedforward, moments_attention, moments_feedforward, new_vectors.T
    )
    delta_v = jnp.pad(new_vectors - outer_vectors[0], ((0, 4), (0, 96)))
    pa, pf, qa, qf, sum_v = groups_sum(delta_a, delta_f, delta_v)
    next_a, next_f, copy_a, copy_f = outer_update(pa, pf, qa, qf, outer_attention, outer_feedforward)
    next_v = outer_step(outer_vectors[0], sum_v[:12, :HW] / 4, outer_vectors[1])
    return (
        block_home,
        grad_home,
        group_a[None],
        group_f[None],
        jnp.stack([owned_vectors, first_vectors, second_vectors])[None],
        group_w[None],
        next_a,
        next_f,
        next_v,
        copy_a,
        copy_f,
        next_v[2].astype(BF),
    )


def solution(mesh):
    shape = dict(mesh.shape)
    fits = shape == {"rep": 4, "fsdp": 8}
    shards = shards_split if fits else shards_generic
    in_specs = (
        P(("rep", "fsdp"), None),
        P(("rep", "fsdp"), None),
        P("rep", None),
        P("rep"),
        P(None, "fsdp", None),
        P(None, "fsdp", None),
        P(None, None, "fsdp"),
        P("rep", None, "fsdp", None),
        P("rep", None, "fsdp", None),
        P("rep", None, None, "fsdp"),
    )
    out_specs = (
        P(("rep", "fsdp"), None),
        P(("rep", "fsdp"), None),
        P("rep", None, "fsdp", None),
        P("rep", None, "fsdp", None),
        P("rep", None, None, "fsdp"),
        P("rep", "fsdp", None),
        P(None, "fsdp", None),
        P(None, "fsdp", None),
        P(None, None, "fsdp"),
        P("fsdp", None),
        P("fsdp", None),
        P(None, "fsdp"),
    )
    return jax.shard_map(shards, mesh=mesh, in_specs=in_specs, out_specs=out_specs, check_vma=False)
```
